32 devices in a mesh: section: 4 (over y, x), mp: 8 (over z, core).
Axes of the slice: x: 2, y: 2, z: 4, core: 2. Of those that a mesh axis runs over, the one named last changes fastest.
Arguments:
- stream: bfloat16 [512, 4096], P(('section', 'mp')), may hold values from -6 to 6
- ffn_gain: float32 [4096], replicated, may hold values from 0.25 to 1.75
- router_weight: bfloat16 [4096, 4], replicated, may hold values from -0.1875 to 0.1875
- expert_ids: int32 [512, 2], P(('section', 'mp')), may hold values from 0 to 3, all different within a row; in each aligned block of 16 rows (0 to 15, 16 to 31, ...) at most 12 rows name the same one
- w_gate: bfloat16 [4, 4096, 14336], P('section', None, 'mp'), may hold values from -0.09375 to 0.09375
- w_up: bfloat16 [4, 4096, 14336], P('section', None, 'mp'), may hold values from -0.09375 to 0.09375
- w_down: bfloat16 [4, 14336, 4096], P('section', 'mp'), may hold values from -0.09375 to 0.09375
- attn_gain: float32 [4096], replicated, may hold values from 0.25 to 1.75
- w_kv: bfloat16 [4096, 2048], P(None, 'mp'), may hold values from -0.09375 to 0.09375
Outputs:
- stream_out: bfloat16 [512, 4096], P(('section', 'mp'))
- kv_decode: bfloat16 [512, 2048], P('section', 'mp')
The draws below stay inside these ranges and needn't reach their ends.
Inputs may be any that keep to these rules, and one draw needn't show every extreme that they name: `expert_ids`: each row names two different experts. Among the rows of one device no expert is named more than 12 times, a bound that some block reaches.
All inputs are finite; a program needn't handle non-finite values.
Results may differ from the reference program's by a relative error of at most 0.02.
Values may be sent and summed in bfloat16 or wider, within the bound.
No kernel may reach another device: no remote copies, remote signals or barrier semaphores. Data moves between devices by JAX's collectives and lax.ppermute only.
A program may use at most 128 MiB of HBM per device.

```python
import math
import jax
import jax.numpy as jnp
import numpy as np
from jax import lax

D = 4096
FF = 14336
TOK_DEV = 16
EXPERTS = 4
CAP = 12
KVW = 2048
TOKENS = 512
N_MP = 8


def steps_of(key, shape, split, least, largest):
    factor_of = 1.0
    for axis_at, shards_of in split:
        draws = jax.random.uniform(jax.random.fold_in(jax.random.fold_in(key, 6), axis_at), (shards_of,), jnp.float32, least / len(split), largest / len(split))
        factor_of = factor_of * jnp.repeat(jnp.exp(draws), shape[axis_at] // shards_of).reshape((-1,) + (1,) * (len(shape) - 1 - axis_at))
    return factor_of


def deal_out(rng, own, number, rows, count, top, reach, skew):
    sequence = jax.random.permutation(rng, count)
    crowded, common = portions_of(count, rows * top, reach, skew, True), portions_of(count, rows * top, reach, skew, False)
    places = jnp.arange(count)

    def named(sizes, turn):
        used = int((sizes > 0).sum())
        fixed = max(1, used // 4)
        moved = fixed + (places - fixed + turn * (used - fixed)) % max(1, count - fixed)
        return jnp.zeros((count,), jnp.int32).at[sequence[jnp.where(places < fixed, places, moved)]].set(jnp.asarray(sizes, jnp.int32))

    sizes = jnp.where(number % 4 == 0, named(crowded, number // 4), named(common, number - number // 4 - 1))
    mixed = jax.random.permutation(jax.random.fold_in(own, 3), count)
    source_of, taker = mixed[0:count // 2 * 2:2], mixed[1:count // 2 * 2:2]
    margin = jnp.minimum(sizes[source_of] - 1, reach - sizes[taker]) // 2
    margin = jnp.where((source_of == sequence[0]) | (taker == sequence[0]) | (sizes[taker] == 0), 0, jnp.maximum(margin, 0))
    moved = jax.random.randint(jax.random.fold_in(own, 4), (count // 2,), 0, 1 << 20) % (margin + 1)
    sizes = sizes.at[source_of].add(-moved).at[taker].add(moved)
    items = jnp.searchsorted(jnp.cumsum(sizes), jnp.arange(rows * top), side="right").astype(jnp.int32)
    listing = items.reshape(top, rows).T
    listing = listing[jax.random.permutation(jax.random.fold_in(own, 1), rows)]
    turn = jax.random.randint(jax.random.fold_in(own, 2), (rows, 1), 0, top)
    return jnp.take_along_axis(listing, (jnp.arange(top)[None, :] + turn) % top, axis=1)


def portions_of(number_of, total, bound, lean, full):
    loads = [(1 << 20) // math.isqrt(rank ** lean) + 1 for rank in range(1, number_of + 1)]
    largest = bound if full else min(bound, max(-(-total // number_of), total * loads[0] // sum(loads)))
    least = 1 if total - largest >= number_of - 1 else 0
    holding, spare = [largest] + [least] * (number_of - 1), total - largest - least * (number_of - 1)
    while spare > 0:
        free = [i for i in range(1, number_of) if holding[i] < largest] or [i for i in range(1, number_of) if holding[i] < bound]
        mass, left = sum([loads[i] for i in free]), spare
        for i in free:
            extra = min(bound - holding[i], max(1, left * loads[i] // mass), spare)
            holding[i] = holding[i] + extra
            spare = spare - extra
    return np.array(holding)


def normal_values(key, extent, scale, limit, cuts=(), kind=jnp.bfloat16):
    entries = jax.random.normal(key, extent, jnp.float32) * scale
    if len(cuts) > 0:
        entries = steps_of(key, extent, cuts, -0.22, 0.18) * entries
    return jnp.clip(entries, min=-limit, max=limit).astype(kind)


def setup_inputs(seed: int = 0) -> dict:
    keys = jax.random.split(jax.random.key(seed), 10)
    stream = normal_values(keys[0], (TOKENS, D), 1.0, 6.0, ((0, 32),))
    ffn_gain = jnp.clip(1.0 + 0.15 * jax.random.normal(keys[1], (D,), jnp.float32), 0.25, 1.75)
    router_weight = normal_values(keys[2], (D, EXPERTS), (D // 4) ** -0.5, 0.1875)
    expert_ids_keys = jax.random.split(jax.random.fold_in(keys[3], 1), TOKENS // TOK_DEV)
    expert_ids_turns = jax.random.permutation(jax.random.fold_in(keys[3], 3), TOKENS // TOK_DEV)
    expert_ids = jax.vmap(lambda own, number: deal_out(jax.random.fold_in(keys[3], 2), own, number, TOK_DEV, EXPERTS, 2, CAP, 2))(expert_ids_keys, expert_ids_turns).reshape((TOKENS, 2))
    w_gate = normal_values(keys[4], (EXPERTS, D, FF), D ** -0.5, 0.09375, ((0, 4), (2, 8)))
    w_up = normal_values(keys[5], (EXPERTS, D, FF), D ** -0.5, 0.09375, ((0, 4), (2, 8)))
    w_down = normal_values(keys[6], (EXPERTS, FF, D), (FF // 4) ** -0.5, 0.09375, ((0, 4), (1, 8)))
    attn_gain = jnp.clip(1.0 + 0.15 * jax.random.normal(keys[7], (D,), jnp.float32), 0.25, 1.75)
    w_kv = normal_values(keys[8], (D, KVW), D ** -0.5, 0.09375, ((1, 8),))
    return dict(stream=stream, ffn_gain=ffn_gain, router_weight=router_weight, expert_ids=expert_ids, w_gate=w_gate, w_up=w_up, w_down=w_down, attn_gain=attn_gain, w_kv=w_kv)


epsilon = 1e-05

def normalize(values, scale_gain):
    floats = values.astype(jnp.float32)
    return floats * lax.rsqrt(lax.optimization_barrier(jnp.mean(floats * floats, axis=-1, keepdims=True)) + epsilon) * scale_gain

def reference(stream, ffn_gain, router_weight, expert_ids, w_gate, w_up, w_down, attn_gain, w_kv):
    tokens = stream.shape[0]
    blocks = tokens // TOK_DEV
    normed = normalize(stream, ffn_gain).astype(jnp.bfloat16)
    logits = jnp.dot(normed, router_weight, preferred_element_type=jnp.float32)
    onehot = expert_ids[:, :, None] == jnp.arange(EXPERTS, dtype=jnp.int32)[None, None, :]
    chosen = lax.optimization_barrier(jnp.sum(jnp.where(onehot, logits[:, None, :], jnp.float32(0.0)), axis=-1))
    share_first = jax.nn.sigmoid(chosen[:, 0] - chosen[:, 1])
    flat_hits = onehot.reshape(blocks, TOK_DEV * 2, EXPERTS).astype(jnp.int32)
    before = jnp.cumsum(flat_hits, axis=1) - flat_hits
    slot_index = lax.optimization_barrier(jnp.sum(before * flat_hits, axis=-1)).reshape(tokens, 2)
    position = (jnp.arange(tokens, dtype=jnp.int32) // TOK_DEV)[:, None] * CAP + slot_index
    repeated = jnp.repeat(normed, 2, axis=0)
    block_width = FF // N_MP
    total = jnp.zeros((tokens, 2, D), jnp.float32)
    for expert in range(EXPERTS):
        target_index = jnp.where(expert_ids == expert, position, blocks * CAP).astype(jnp.int32)
        buffer = jnp.zeros((blocks * CAP, D), jnp.bfloat16).at[target_index.reshape(-1)].set(repeated, mode='drop')
        gate_part = jnp.dot(buffer, w_gate[expert], preferred_element_type=jnp.float32)
        up_part = jnp.dot(buffer, w_up[expert], preferred_element_type=jnp.float32)
        hidden = (jax.nn.silu(gate_part) * up_part).astype(jnp.bfloat16)
        hidden_blocks = hidden.reshape(blocks * CAP, N_MP, block_width).transpose(1, 0, 2)
        down_blocks = w_down[expert].reshape(N_MP, block_width, D)

        def add_block(carry, pair):
            product = jnp.dot(pair[0], pair[1], preferred_element_type=jnp.float32)
            rounded = lax.optimization_barrier(product.astype(jnp.bfloat16))
            return (carry + rounded.astype(jnp.float32), None)
        summed, unused = lax.scan(add_block, jnp.zeros((blocks * CAP, D), jnp.float32), (hidden_blocks, down_blocks))
        result_rows = summed.astype(jnp.bfloat16)
        safe_index = jnp.clip(target_index, 0, blocks * CAP - 1)
        picked = result_rows[safe_index.reshape(-1)].reshape(tokens, 2, D).astype(jnp.float32)
        total = total + jnp.where((expert_ids == expert)[:, :, None], picked, jnp.float32(0.0))
    updated = stream.astype(jnp.float32) + share_first[:, None] * total[:, 0] + (1.0 - share_first)[:, None] * total[:, 1]
    stream_out = updated.astype(jnp.bfloat16)
    attn_input = normalize(stream_out, attn_gain).astype(jnp.bfloat16)
    kv_local = jnp.dot(attn_input, w_kv, preferred_element_type=jnp.float32).astype(jnp.bfloat16)
    kv_decode = jnp.roll(kv_local, TOK_DEV * N_MP, axis=0)
    return (stream_out, kv_decode)
```

```python
import functools

import jax
import jax.numpy as jnp
from jax import lax
from jax.experimental import pallas as pl
from jax.experimental.pallas import tpu as pltpu
from jax.sharding import PartitionSpec as P

epsilon = 1e-05
META = 128
IN_CHUNKS = 2
OUT_CHUNKS = 2
BF = jnp.bfloat16
F32 = jnp.float32


def swap(value, axis, mask):
    count = lax.axis_size(axis)
    return lax.ppermute(value, axis, [(i, i ^ mask) for i in range(count)])


def call(kernel, outs, *args, smem=0, vmem=None, cost=None):
    specs = [
        pl.BlockSpec(memory_space=pltpu.SMEM if i < smem else pltpu.VMEM)
        for i in range(len(args))
    ]
    return pl.pallas_call(
        kernel,
        out_shape=outs,
        in_specs=specs,
        out_specs=jax.tree.map(lambda _: pl.BlockSpec(memory_space=pltpu.VMEM), outs),
        compiler_params=pltpu.CompilerParams(vmem_limit_bytes=vmem),
        cost_estimate=cost,
    )(*args)


def shape(rows, cols, dtype=BF):
    return jax.ShapeDtypeStruct((rows, cols), dtype)


def prep_kernel(pos_ref, stream_ref, gain_ref, router_ref, ids_ref, *out_refs):
    section = pos_ref[0]
    rows = stream_ref.shape[0]
    x = stream_ref[...].astype(F32)
    scale = lax.rsqrt(jnp.mean(x * x, axis=-1, keepdims=True) + epsilon)
    normed = (x * scale * gain_ref[...]).astype(BF)
    logits = lax.dot_general(
        normed, router_ref[...], (((1,), (1,)), ((), ())), preferred_element_type=F32
    )
    experts = logits.shape[1]
    row_at = lax.broadcasted_iota(jnp.int32, (rows, rows), 0)
    lane_at = lax.broadcasted_iota(jnp.int32, (rows, rows), 1)
    a_row = jnp.broadcast_to(ids_ref[0:1, :], (rows, rows))
    b_row = jnp.broadcast_to(ids_ref[1:2, :], (rows, rows))

    def total(v):
        return jnp.sum(v.astype(F32), axis=1, keepdims=True)

    def column(r):
        return total(jnp.where(row_at == lane_at, r, 0)).astype(jnp.int32)

    a_col, b_col = column(a_row), column(b_row)
    earlier = lane_at < row_at

    def slots(col):
        c = jnp.broadcast_to(col, (rows, rows))
        return total(jnp.where(earlier & (a_row == c), 1, 0)) + total(
            jnp.where(earlier & (b_row == c), 1, 0)
        )

    expert_at = lax.broadcasted_iota(jnp.int32, (rows, experts), 1)
    chosen_a = jnp.sum(jnp.where(expert_at == a_col, logits, 0.0), axis=1, keepdims=True)
    chosen_b = jnp.sum(jnp.where(expert_at == b_col, logits, 0.0), axis=1, keepdims=True)
    share = jax.nn.sigmoid(chosen_a - chosen_b)
    share_hi = share.astype(BF).astype(F32)
    parts = [
        (a_col ^ section).astype(F32),
        slots(a_col),
        (b_col ^ section).astype(F32),
        slots(b_col),
        share_hi,
        share - share_hi,
    ]
    at = lax.broadcasted_iota(jnp.int32, (rows, META), 1)
    meta = jnp.zeros((rows, META), F32)
    for i, part in enumerate(parts):
        meta = jnp.where(at == i, part, meta)
    width = stream_ref.shape[1] // len(out_refs)
    for k, out in enumerate(out_refs):
        out[:, :width] = normed[:, k * width : (k + 1) * width]
    out_refs[0][:, width:] = meta.astype(BF)


def targets(meta, block, cap, blocks):
    at = lax.broadcasted_iota(jnp.int32, meta.shape, 1)

    def pick(i):
        return jnp.sum(jnp.where(at == i, meta, 0.0), axis=1, keepdims=True)

    def place(i):
        return (pick(i) * (blocks * cap) + pick(i + 1)).astype(jnp.int32) + block * cap

    return place(0), place(2), pick(4) + pick(5)


def dispatch_kernel(cap, width, n_blocks, *refs):
    metas, xs, outs = refs[:n_blocks], refs[n_blocks : 2 * n_blocks], refs[2 * n_blocks :]
    slots = n_blocks * cap
    tables = []
    for k in range(n_blocks):
        meta = metas[k][:, metas[k].shape[1] - META :].astype(F32)
        first, second, _ = targets(meta, k, cap, n_blocks)
        at = lax.broadcasted_iota(jnp.int32, (meta.shape[0], slots * len(outs)), 1)
        tables.append(jnp.where((at == first) | (at == second), 1.0, 0.0))
    table = jnp.concatenate(tables, axis=0).astype(BF)
    tokens = jnp.concatenate([x[:, :width] for x in xs], axis=0)
    rows = lax.dot_general(
        table, tokens, (((0,), (0,)), ((), ())), preferred_element_type=F32
    ).astype(BF)
    for j, out in enumerate(outs):
        out[...] = rows[j * slots : (j + 1) * slots]


def gate_up_kernel(n_x, has_acc, last, *refs):
    xs, rest = refs[:n_x], refs[n_x:]
    gate_ref, up_ref = rest[:2]
    rest = rest[2:]
    if has_acc:
        acc_gate, acc_up = rest[:2]
        rest = rest[2:]
    outs, x_all = rest[:-1], rest[-1]

    @pl.when(pl.program_id(0) == 0)
    def _():
        rows = xs[0].shape[0]
        for i, x in enumerate(xs):
            x_all[i * rows : (i + 1) * rows, :] = x[...]

    x = x_all[...]
    gate = jnp.dot(x, gate_ref[...], preferred_element_type=F32)
    up = jnp.dot(x, up_ref[...], preferred_element_type=F32)
    if has_acc:
        gate = gate + acc_gate[...]
        up = up + acc_up[...]
    if last:
        outs[0][...] = (gate / (1.0 + jnp.exp(-gate)) * up).astype(BF)
    else:
        outs[0][...] = gate
        outs[1][...] = up


def gate_up(xs, w_gate, w_up, acc, chunk, last):
    hidden = w_gate.shape[1]
    rows, width = xs[0].shape
    total = rows * len(xs)
    tile = 256 if hidden % 256 == 0 else hidden
    weight = pl.BlockSpec((width, tile), lambda n: (chunk, n))
    column = pl.BlockSpec((total, tile), lambda n: (0, n))
    outs = [shape(total, hidden, BF)] if last else [shape(total, hidden, F32)] * 2
    return pl.pallas_call(
        functools.partial(gate_up_kernel, len(xs), acc is not None, last),
        out_shape=outs,
        grid=(hidden // tile,),
        in_specs=[pl.BlockSpec((rows, width), lambda n: (0, 0))] * len(xs)
        + [weight, weight]
        + ([column, column] if acc is not None else []),
        out_specs=[column] * len(outs),
        scratch_shapes=[pltpu.VMEM((total, width), BF)],
        compiler_params=pltpu.CompilerParams(vmem_limit_bytes=48 * 2**20),
        cost_estimate=pl.CostEstimate(
            flops=4 * total * width * hidden, bytes_accessed=4 * width * hidden, transcendentals=0
        ),
    )(*xs, w_gate, w_up, *(acc or []))


def down_kernel(hidden_ref, w_ref, own_ref, other_ref):
    y = jnp.dot(hidden_ref[...], w_ref[...], preferred_element_type=F32).astype(BF)
    half = own_ref.shape[0]
    own_ref[...] = y[:half]
    other_ref[...] = y[half:]


def down(hidden, w_down, chunk, width):
    total, inner = hidden.shape
    tile = min(256, width)
    steps = width // tile
    half = total // 2
    return pl.pallas_call(
        down_kernel,
        out_shape=[shape(half, width)] * 2,
        grid=(steps,),
        in_specs=[
            pl.BlockSpec((total, inner), lambda n: (0, 0)),
            pl.BlockSpec((inner, tile), lambda n: (0, chunk * steps + n)),
        ],
        out_specs=[pl.BlockSpec((half, tile), lambda n: (0, n))] * 2,
        compiler_params=pltpu.CompilerParams(vmem_limit_bytes=48 * 2**20),
        cost_estimate=pl.CostEstimate(
            flops=2 * total * inner * width, bytes_accessed=2 * inner * width, transcendentals=0
        ),
    )(hidden, w_down)


def core_sum_kernel(a_ref, b_ref, *outs):
    rows = outs[0].shape[0]
    for j, out in enumerate(outs):
        at = slice(j * rows, (j + 1) * rows)
        out[...] = (a_ref[at, :].astype(F32) + b_ref[at, :].astype(F32)).astype(BF)


def mix_kernel(cap, n_blocks, n_rows, *refs):
    metas, rows = refs[:n_blocks], refs[n_blocks : n_blocks + n_rows]
    outs = refs[n_blocks + n_rows :]
    results = jnp.concatenate([r[...] for r in rows], axis=0)
    highs, lows = [], []
    for k in range(n_blocks):
        meta = metas[k][:, metas[k].shape[1] - META :].astype(F32)
        first, second, share = targets(meta, k, cap, n_blocks)
        at = lax.broadcasted_iota(jnp.int32, (meta.shape[0], results.shape[0]), 1)
        weight = jnp.where(at == first, share, 0.0) + jnp.where(at == second, 1.0 - share, 0.0)
        high = weight.astype(BF).astype(F32)
        highs.append(high)
        lows.append(weight - high)
    high = jnp.concatenate(highs, axis=0).astype(BF)
    low = jnp.concatenate(lows, axis=0).astype(BF)
    mixed = jnp.dot(high, results, preferred_element_type=F32) + jnp.dot(
        low, results, preferred_element_type=F32
    )
    count = outs[0].shape[0]
    for k, out in enumerate(outs):
        out[...] = mixed[k * count : (k + 1) * count].astype(BF)


def update_kernel(chunk, stream_ref, *refs):
    out = refs[-1]
    width = out.shape[1]
    value = stream_ref[:, chunk * width : (chunk + 1) * width].astype(F32)
    for part in refs[:-1]:
        value = value + part[...].astype(F32)
    out[...] = value.astype(BF)


def kv_kernel(n_chunks, pos_ref, gain_ref, w_ref, *refs):
    out = refs[-1]
    blocks = refs[:-1]
    per = len(blocks) // n_chunks
    width = blocks[0].shape[1]
    count = blocks[0].shape[0]
    squares = None
    total = None
    for k in range(n_chunks):
        x = jnp.concatenate([b[...] for b in blocks[k * per : (k + 1) * per]], axis=0).astype(F32)
        part = jnp.sum(x * x, axis=-1, keepdims=True)
        squares = part if squares is None else squares + part
        at = slice(k * width, (k + 1) * width)
        product = jnp.dot(
            (x * gain_ref[:, at]).astype(BF), w_ref[at, :], preferred_element_type=F32
        )
        total = product if total is None else total + product
    scale = lax.rsqrt(squares / (width * n_chunks) + epsilon)
    result = (total * scale).astype(BF)
    member = pos_ref[1]
    for i in range(per):
        out[pl.ds(pl.multiple_of((member ^ i) * count, count), count), :] = result[
            i * count : (i + 1) * count
        ]


def body(stream, ffn_gain, router_weight, expert_ids, w_gate, w_up, w_down, attn_gain, w_kv):
    rows, model = stream.shape
    experts = router_weight.shape[1]
    cap = min(rows, 3 * rows // experts)
    sections, members = lax.axis_size("section"), lax.axis_size("mp")
    cores = 2
    zs = members // cores
    pos = jnp.stack([lax.axis_index("section"), lax.axis_index("mp")]).astype(jnp.int32)
    width = model // IN_CHUNKS
    chunks = call(
        prep_kernel,
        [shape(rows, width + (META if k == 0 else 0)) for k in range(IN_CHUNKS)],
        pos,
        stream,
        ffn_gain.reshape(1, model),
        router_weight.T,
        expert_ids.T,
        smem=1,
    )
    gathered = [
        [own] + [swap(own, "mp", k * cores) for k in range(1, zs)] for own in chunks
    ]
    metas = gathered[0]
    acc = None
    for k in range(IN_CHUNKS):
        sent = call(
            functools.partial(dispatch_kernel, cap, width, zs),
            [shape(zs * cap, width)] * sections,
            *metas,
            *gathered[k],
        )
        mine = [sent[0]] + [swap(sent[j], "section", j) for j in range(1, sections)]
        others = [swap(v, "mp", 1) for v in mine]
        acc = gate_up(mine + others, w_gate[0], w_up[0], acc, k, k == IN_CHUNKS - 1)
    hidden = acc[0]
    width = model // OUT_CHUNKS
    outs, blocks = [], []
    for k in range(OUT_CHUNKS):
        own, other = down(hidden, w_down[0], k, width)
        other = swap(other, "mp", 1)
        parts = call(core_sum_kernel, [shape(zs * cap, width)] * sections, own, other)
        returned = [parts[0]] + [swap(parts[j], "section", j) for j in range(1, sections)]
        mixed = call(
            functools.partial(mix_kernel, cap, zs, sections),
            [shape(rows, width)] * zs,
            *metas,
            *returned,
        )
        arrived = [mixed[0]] + [swap(mixed[j], "mp", j * cores) for j in range(1, zs)]
        new = call(
            functools.partial(update_kernel, k), shape(rows, width), stream, *arrived
        )
        outs.append(new)
        mine = [new] + [swap(new, "mp", j * cores) for j in range(1, zs)]
        both = [[v, swap(v, "mp", 1)] for v in mine]
        blocks += [v for pair in both for v in pair]
    kv_local = call(
        functools.partial(kv_kernel, OUT_CHUNKS),
        shape(members * rows, w_kv.shape[1]),
        pos,
        attn_gain.reshape(1, model),
        w_kv,
        *blocks,
        smem=1,
    )
    stream_out = jnp.concatenate(outs, axis=1)
    pairs = [(i, (i + 1) % sections) for i in range(sections)]
    return stream_out, lax.ppermute(kv_local, "section", pairs)


def solution(mesh):
    in_specs = (
        P(("section", "mp"), None),
        P(),
        P(),
        P(("section", "mp"), None),
        P("section", None, "mp"),
        P("section", None, "mp"),
        P("section", "mp", None),
        P(),
        P(None, "mp"),
    )
    out_specs = (P(("section", "mp"), None), P("section", "mp"))
    return jax.shard_map(body, mesh=mesh, in_specs=in_specs, out_specs=out_specs, check_vma=False)
```

```python
import functools

import jax
import jax.numpy as jnp
from jax import lax
from jax.experimental import pallas as pl
from jax.experimental.pallas import tpu as pltpu
from jax.sharding import PartitionSpec as P

epsilon = 1e-05
META = 128
CHUNKS = 2
BF = jnp.bfloat16
F32 = jnp.float32


def swap(value, axis, mask):
    count = lax.axis_size(axis)
    return lax.ppermute(value, axis, [(i, i ^ mask) for i in range(count)])


def call(kernel, outs, *args, vmem=6 * 2**20, cost=None, scratch=(), hbm=()):
    specs = [pl.BlockSpec(memory_space=pltpu.VMEM)] * len(args)
    specs += [pl.BlockSpec(memory_space=pl.ANY)] * len(hbm)
    return pl.pallas_call(
        kernel,
        out_shape=outs,
        in_specs=specs,
        out_specs=jax.tree.map(lambda _: pl.BlockSpec(memory_space=pltpu.VMEM), outs),
        scratch_shapes=list(scratch),
        compiler_params=pltpu.CompilerParams(vmem_limit_bytes=vmem),
        cost_estimate=cost,
    )(*args, *hbm)


def shape(rows, cols, dtype=BF):
    return jax.ShapeDtypeStruct((rows, cols), dtype)


def prep_kernel(stream_ref, gain_ref, router_ref, ids_ref, out_ref):
    section = lax.axis_index("section")
    rows = stream_ref.shape[0]
    x = stream_ref[...].astype(F32)
    scale = lax.rsqrt(jnp.mean(x * x, axis=-1, keepdims=True) + epsilon)
    normed = (x * scale * gain_ref[...]).astype(BF)
    logits = lax.dot_general(
        normed, router_ref[...], (((1,), (1,)), ((), ())), preferred_element_type=F32
    )
    experts = logits.shape[1]
    row_at = lax.broadcasted_iota(jnp.int32, (rows, rows), 0)
    lane_at = lax.broadcasted_iota(jnp.int32, (rows, rows), 1)
    a_row = jnp.broadcast_to(ids_ref[0:1, :], (rows, rows))
    b_row = jnp.broadcast_to(ids_ref[1:2, :], (rows, rows))

    def total(v):
        return jnp.sum(v.astype(F32), axis=1, keepdims=True)

    def column(r):
        return total(jnp.where(row_at == lane_at, r, 0)).astype(jnp.int32)

    a_col, b_col = column(a_row), column(b_row)
    earlier = lane_at < row_at

    def slots(col):
        c = jnp.broadcast_to(col, (rows, rows))
        return total(jnp.where(earlier & (a_row == c), 1, 0)) + total(
            jnp.where(earlier & (b_row == c), 1, 0)
        )

    expert_at = lax.broadcasted_iota(jnp.int32, (rows, experts), 1)
    chosen_a = jnp.sum(jnp.where(expert_at == a_col, logits, 0.0), axis=1, keepdims=True)
    chosen_b = jnp.sum(jnp.where(expert_at == b_col, logits, 0.0), axis=1, keepdims=True)
    share = jax.nn.sigmoid(chosen_a - chosen_b)
    share_hi = share.astype(BF).astype(F32)
    parts = [
        (a_col ^ section).astype(F32),
        slots(a_col),
        (b_col ^ section).astype(F32),
        slots(b_col),
        share_hi,
        share - share_hi,
    ]
    at = lax.broadcasted_iota(jnp.int32, (rows, META), 1)
    meta = jnp.zeros((rows, META), F32)
    for i, part in enumerate(parts):
        meta = jnp.where(at == i, part, meta)
    width = stream_ref.shape[1]
    out_ref[:, :width] = normed
    out_ref[:, width:] = meta.astype(BF)


def targets(meta, block, cap, blocks):
    at = lax.broadcasted_iota(jnp.int32, meta.shape, 1)

    def pick(i):
        return jnp.sum(jnp.where(at == i, meta, 0.0), axis=1, keepdims=True)

    def place(i):
        return (pick(i) * (blocks * cap) + pick(i + 1)).astype(jnp.int32) + block * cap

    return place(0), place(2), pick(4) + pick(5)


def dispatch_kernel(cap, width, n_blocks, *refs):
    xs, outs = refs[:n_blocks], refs[n_blocks:]
    slots = n_blocks * cap
    sections = len(outs) // CHUNKS
    tables = []
    for k in range(n_blocks):
        meta = xs[k][:, width:].astype(F32)
        first, second, _ = targets(meta, k, cap, n_blocks)
        at = lax.broadcasted_iota(jnp.int32, (meta.shape[0], slots * sections), 1)
        tables.append(jnp.where((at == first) | (at == second), 1.0, 0.0))
    table = jnp.concatenate(tables, axis=0).astype(BF)
    tokens = jnp.concatenate([x[:, :width] for x in xs], axis=0)
    rows = lax.dot_general(
        table, tokens, (((0,), (0,)), ((), ())), preferred_element_type=F32
    ).astype(BF)
    part = width // CHUNKS
    for i, out in enumerate(outs):
        k, j = divmod(i, sections)
        out[...] = rows[j * slots : (j + 1) * slots, k * part : (k + 1) * part]


def columns(n, tile):
    return pl.ds(n * tile, tile)


def fetch(src, dst, sems, rows, first, tile):
    copies = []
    for n in range(dst.shape[1] // tile):
        copies.append(
            pltpu.make_async_copy(
                src.at[rows, pl.ds(first + n * tile, tile)], dst.at[:, columns(n, tile)], sems.at[n]
            )
        )
        copies[-1].start()
    return copies


def stack(xs, x_all):
    rows = xs[0].shape[0]
    for i, x in enumerate(xs):
        x_all[i * rows : (i + 1) * rows, :] = x[...]


def first_kernel(n_x, tile, *refs):
    xs, (gate_hbm, up_hbm, out_gate, out_up, x_all, gate_w, up_w, sems) = refs[:n_x], refs[n_x:]
    rows = pl.ds(0, gate_w.shape[0])
    gates = fetch(gate_hbm, gate_w, sems.at[0], rows, 0, tile)
    ups = fetch(up_hbm, up_w, sems.at[1], rows, 0, tile)
    stack(xs, x_all)
    for n in range(len(gates)):
        at = columns(n, tile)
        for copies, w, out in ((gates, gate_w, out_gate), (ups, up_w, out_up)):
            copies[n].wait()
            out[:, at] = jnp.dot(x_all[...], w[:, at], preferred_element_type=F32)


def second_kernel(n_x, tile, step, *refs):
    xs, rest = refs[:n_x], refs[n_x:]
    acc_gate, acc_up, gate_hbm, up_hbm, down_hbm, hidden, own, other = rest[:8]
    x_all, gate_w, up_w, down_w, sems, down_sems = rest[8:]
    depth = gate_w.shape[0]
    rows = pl.ds(depth, depth)
    gates = fetch(gate_hbm, gate_w, sems.at[0], rows, 0, tile)
    ups = fetch(up_hbm, up_w, sems.at[1], rows, 0, tile)
    downs = fetch(down_hbm, down_w, down_sems, slice(None), 0, step)
    stack(xs, x_all)
    for n in range(len(gates)):
        at = columns(n, tile)
        gates[n].wait()
        ups[n].wait()
        gate = acc_gate[:, at] + jnp.dot(x_all[...], gate_w[:, at], preferred_element_type=F32)
        up = acc_up[:, at] + jnp.dot(x_all[...], up_w[:, at], preferred_element_type=F32)
        hidden[:, at] = (gate / (1.0 + jnp.exp(-gate)) * up).astype(BF)
    project(hidden, downs, down_w, own, other, step)


def project(hidden, downs, down_w, own, other, step):
    half = own.shape[0]
    for n in range(len(downs)):
        at = columns(n, step)
        downs[n].wait()
        y = jnp.dot(hidden[...], down_w[:, at], preferred_element_type=F32).astype(BF)
        own[:, at] = y[:half]
        other[:, at] = y[half:]


def third_kernel(step, hidden, down_hbm, own, other, down_w, down_sems):
    downs = fetch(down_hbm, down_w, down_sems, slice(None), own.shape[1], step)
    project(hidden, downs, down_w, own, other, step)


BIG = 44 * 2**20


def ffn(xs, w_gate, w_up, w_down):
    model, inner = w_gate.shape
    rows, depth = xs[0][0].shape
    total = rows * len(xs[0])
    width = model - depth
    wide = 896 if inner % 896 == 0 else inner
    tile = 256 if inner % 256 == 0 else inner
    step = 512
    dma = pltpu.SemaphoreType.DMA
    halves = [pltpu.VMEM((depth, inner), BF)] * 2
    flops = total * inner * model

    def cost(part):
        return pl.CostEstimate(
            flops=part * flops, bytes_accessed=part * model * inner, transcendentals=0
        )

    acc = call(
        functools.partial(first_kernel, len(xs[0]), wide),
        [shape(total, inner, F32)] * 2,
        *xs[0],
        hbm=(w_gate, w_up),
        scratch=[pltpu.VMEM((total, depth), BF), *halves, dma((2, inner // wide))],
        vmem=BIG,
        cost=cost(2),
    )
    hidden, own0, other0 = call(
        functools.partial(second_kernel, len(xs[1]), tile, step),
        [shape(total, inner), *[shape(total // 2, width)] * 2],
        *xs[1],
        *acc,
        hbm=(w_gate, w_up, w_down),
        scratch=[
            pltpu.VMEM((total, depth), BF),
            *halves,
            pltpu.VMEM((inner, width), BF),
            dma((2, inner // tile)),
            dma((width // step,)),
        ],
        vmem=BIG,
        cost=cost(3),
    )
    own1, other1 = call(
        functools.partial(third_kernel, step),
        [shape(total // 2, width)] * 2,
        hidden,
        hbm=(w_down,),
        scratch=[pltpu.VMEM((inner, width), BF), dma((width // step,))],
        vmem=BIG,
        cost=cost(1),
    )
    return [(own0, other0), (own1, other1)]


def core_sum_kernel(a_ref, b_ref, *outs):
    rows = outs[0].shape[0]
    for j, out in enumerate(outs):
        at = slice(j * rows, (j + 1) * rows)
        out[...] = (a_ref[at, :].astype(F32) + b_ref[at, :].astype(F32)).astype(BF)


def mix_kernel(cap, n_blocks, n_rows, *refs):
    metas, rows = refs[:n_blocks], refs[n_blocks : n_blocks + n_rows]
    outs = refs[n_blocks + n_rows :]
    results = jnp.concatenate([r[...] for r in rows], axis=0)
    highs, lows = [], []
    for k in range(n_blocks):
        meta = metas[k][:, metas[k].shape[1] - META :].astype(F32)
        first, second, share = targets(meta, k, cap, n_blocks)
        at = lax.broadcasted_iota(jnp.int32, (meta.shape[0], results.shape[0]), 1)
        weight = jnp.where(at == first, share, 0.0) + jnp.where(at == second, 1.0 - share, 0.0)
        high = weight.astype(BF).astype(F32)
        highs.append(high)
        lows.append(weight - high)
    high = jnp.concatenate(highs, axis=0).astype(BF)
    low = jnp.concatenate(lows, axis=0).astype(BF)
    mixed = jnp.dot(high, results, preferred_element_type=F32) + jnp.dot(
        low, results, preferred_element_type=F32
    )
    count = outs[0].shape[0]
    for k, out in enumerate(outs):
        out[...] = mixed[k * count : (k + 1) * count].astype(BF)


def update_kernel(chunk, last, n_parts, stream_ref, *refs):
    count = n_parts + chunk * last
    parts, earlier, out = refs[:n_parts], refs[n_parts:count], refs[count]
    width = out.shape[1]
    value = stream_ref[:, chunk * width : (chunk + 1) * width].astype(F32)
    for part in parts:
        value = value + part[...].astype(F32)
    value = value.astype(BF)
    out[...] = value
    for whole in refs[count + 1 :]:
        for k, v in enumerate(earlier):
            whole[:, k * width : (k + 1) * width] = v[...]
        whole[:, chunk * width :] = value


def kv_kernel(n_chunks, gain_ref, w_ref, *refs):
    blocks, out = refs[:-1], refs[-1]
    per = len(blocks) // n_chunks
    width = blocks[0].shape[1]
    count = blocks[0].shape[0]
    squares = None
    total = None
    for k in range(n_chunks):
        x = jnp.concatenate([b[...] for b in blocks[k * per : (k + 1) * per]], axis=0).astype(F32)
        part = jnp.sum(x * x, axis=-1, keepdims=True)
        squares = part if squares is None else squares + part
        at = slice(k * width, (k + 1) * width)
        product = jnp.dot(
            (x * gain_ref[:, at]).astype(BF), w_ref[at, :], preferred_element_type=F32
        )
        total = product if total is None else total + product
    scale = lax.rsqrt(squares / (width * n_chunks) + epsilon)
    result = (total * scale).astype(BF)
    member = lax.axis_index("mp")
    for i in range(per):
        out[pl.ds(pl.multiple_of((member ^ i) * count, count), count), :] = result[
            i * count : (i + 1) * count
        ]


def body(stream, ffn_gain, router_weight, expert_ids, w_gate, w_up, w_down, attn_gain, w_kv):
    rows, model = stream.shape
    experts = router_weight.shape[1]
    cap = min(rows, 3 * rows // experts)
    sections, members = lax.axis_size("section"), lax.axis_size("mp")
    cores = 2
    zs = members // cores
    own = call(
        prep_kernel,
        shape(rows, model + META),
        stream,
        ffn_gain.reshape(1, model),
        router_weight.T,
        expert_ids.T,
    )
    gathered = [own] + [swap(own, "mp", k * cores) for k in range(1, zs)]
    width = model // CHUNKS
    sent = call(
        functools.partial(dispatch_kernel, cap, model, zs),
        [shape(zs * cap, width)] * (CHUNKS * sections),
        *gathered,
    )
    xs = []
    for k in range(CHUNKS):
        mine = [sent[k * sections]]
        mine += [swap(sent[k * sections + j], "section", j) for j in range(1, sections)]
        xs.append(mine + [swap(v, "mp", 1) for v in mine])
    metas = [m[:, model:] for m in gathered]
    blocks, news = [], []
    for k, (own, other) in enumerate(ffn(xs, w_gate[0], w_up[0], w_down[0])):
        sums = call(
            core_sum_kernel, [shape(zs * cap, width)] * sections, own, swap(other, "mp", 1)
        )
        returned = [sums[0]] + [swap(sums[j], "section", j) for j in range(1, sections)]
        mixed = call(
            functools.partial(mix_kernel, cap, zs, sections),
            [shape(rows, width)] * zs,
            *metas,
            *returned,
        )
        arrived = [mixed[0]] + [swap(mixed[j], "mp", j * cores) for j in range(1, zs)]
        last = k == CHUNKS - 1
        new, *stream_out = call(
            functools.partial(update_kernel, k, last, zs),
            [shape(rows, width)] + [shape(rows, model)] * last,
            stream,
            *arrived,
            *(news if last else []),
        )
        news.append(new)
        for j in range(zs):
            pairs = [
                (s * members + m, (s + 1) % sections * members + (m ^ (j * cores)))
                for s in range(sections)
                for m in range(members)
            ]
            block = lax.ppermute(new, ("section", "mp"), pairs)
            blocks += [block, swap(block, "mp", 1)]
    kv_decode = call(
        functools.partial(kv_kernel, CHUNKS),
        shape(members * rows, w_kv.shape[1]),
        attn_gain.reshape(1, model),
        w_kv,
        *blocks,
    )
    return stream_out[0], kv_decode


def solution(mesh):
    in_specs = (
        P(("section", "mp"), None),
        P(),
        P(),
        P(("section", "mp"), None),
        P("section", None, "mp"),
        P("section", None, "mp"),
        P("section", "mp", None),
        P(),
        P(None, "mp"),
    )
    out_specs = (P(("section", "mp"), None), P("section", "mp"))
    return jax.shard_map(body, mesh=mesh, in_specs=in_specs, out_specs=out_specs, check_vma=False)
```
